32 devices in a mesh: dp: 4 (over z), head: 2 (over y), tok: 4 (over x, core).
Axes of the slice: x: 2, y: 2, z: 4, core: 2. Of those that a mesh axis runs over, the one named last changes fastest.
Arguments:
- mamba_input: bfloat16 [8, 64, 2048], P('dp', 'tok', 'head'), may hold values from -6 to 6
- gate_input: bfloat16 [8, 64, 2048], P('dp', 'tok', 'head'), may hold values from -6 to 6
- in_b: bfloat16 [8, 64, 256], P('dp', 'tok', 'head'), may hold values from -0.75 to 0.75
- in_c: bfloat16 [8, 64, 256], P('dp', 'tok', 'head'), may hold values from -0.75 to 0.75
- step_size: bfloat16 [8, 64, 32], P('dp', 'tok', 'head'), may hold values from 0.019897461 to 1
- decay_rate: float32 [32], P('head'), may hold values from 0.01 to 1
- skip_weight: float32 [32], P('head'), may hold values from 0.5 to 1.5
- norm_gain: float32 [2048], P('head'), may hold values from 0.1 to 1.9
- ssm_state: bfloat16 [8, 32, 64, 128], P('dp', 'head', None, 'tok'), may hold values from -6 to 6
- out_weight: bfloat16 [2048, 4096], P(('head', 'tok')), may hold values from -0.125 to 0.125
- queries: bfloat16 [8, 64, 1024], P('dp', 'tok', 'head'), may hold values from -6 to 6
- draft_token_keys: bfloat16 [8, 64, 256], P('dp', 'tok', 'head'), may hold values from -6 to 6
- draft_values: bfloat16 [8, 64, 256], P('dp', 'tok', 'head'), may hold values from -6 to 6
- cached_key_rows: bfloat16 [8, 4096, 256], P('dp', 'tok', 'head'), may hold values from -4 to 4
- cache_values: bfloat16 [8, 4096, 256], P('dp', 'tok', 'head'), may hold values from -6 to 6
- cache_len: int32 [8], P('dp'), may hold values from 2 to 4096
- accepted: int32 [8], P('dp'), may hold values from 0 to 64
Outputs:
- mamba_out: bfloat16 [64, 8, 4096], P(('head', 'tok'), 'dp')
- attn_context: bfloat16 [8, 64, 1024], P('dp', 'tok', 'head')
- committed_state: bfloat16 [8, 32, 64, 128], P('dp', 'head', None, 'tok')
The draws below stay inside these ranges and needn't reach their ends.
Inputs may be any that keep to these rules, and one draw needn't show every extreme that they name: Each sequence's cached positions 0 to cache_len - 1 are valid.
All inputs are finite; a program needn't handle non-finite values.
Results may differ from the reference program's by a relative error of at most 0.018.
Values may be sent and summed in bfloat16 or wider, within the bound.
A program may use at most 64 MiB of HBM per device.

```python
import math
import jax
import jax.numpy as jnp
from jax import lax

D = 4096
STATE = 128
HEAD_DIM = 64
ATT_DIM = 128
HEADS = 32
GROUPS = 2
QHEADS = 8
KVHEADS = 2
DRAFT = 64
CACHE = 4096
BATCH = 8
N_HEAD = 2
N_TOK = 4


def draw_queries(key, part):
    shape = (BATCH, DRAFT, QHEADS * ATT_DIM)
    base = jnp.clip(jax.random.normal(jax.random.fold_in(key, 11), shape), -4.0, 4.0)
    return base.astype(jnp.bfloat16)


def draw_cached_key_rows(key, part):
    shape = (BATCH, CACHE, KVHEADS * ATT_DIM)
    base = jnp.clip(jax.random.normal(jax.random.fold_in(key, 21), shape), -4.0, 4.0)
    return base.astype(jnp.bfloat16)


def with_ends(result, rng, low, top_value):
    shape = result.shape
    place = [jax.random.randint(jax.random.fold_in(rng, axis), (), 0, shape[axis]) for axis in range(len(shape))]
    result = result.at[tuple(place)].set(low)
    longest = shape.index(max(shape))
    place[longest] = (place[longest] + 1) % shape[longest]
    return result.at[tuple(place)].set(top_value)


def level_of(key, extent, shards, least, high):
    factor_of = 1.0
    for dim, parts in shards:
        steps = jax.random.uniform(jax.random.fold_in(jax.random.fold_in(key, 6), dim), (parts,), jnp.float32, least / len(shards), high / len(shards))
        factor_of = factor_of * jnp.repeat(jnp.exp(steps), extent[dim] // parts).reshape((-1,) + (1,) * (len(extent) - 1 - dim))
    return factor_of


def scatter_about(rng, shape, deviation, bound, cuts=(), dtype=jnp.bfloat16):
    values = deviation * jax.random.normal(rng, shape, jnp.float32)
    if cuts:
        values = values * level_of(rng, shape, cuts, -0.22, 0.18)
    return jnp.clip(values, -bound, bound).astype(dtype)


def setup_inputs(seed: int = 0) -> dict:
    key_of = jax.random.split(jax.random.key(seed), 18)
    return {
        "mamba_input": scatter_about(key_of[0], (BATCH, DRAFT, HEADS * HEAD_DIM), 1.0, 6.0, ((0, 4), (1, 4), (2, 2))),
        "gate_input": scatter_about(key_of[1], (BATCH, DRAFT, HEADS * HEAD_DIM), 1.0, 6.0, ((0, 4), (1, 4), (2, 2))),
        "in_b": scatter_about(key_of[2], (BATCH, DRAFT, GROUPS * STATE), 0.125, 0.75, ((0, 4), (1, 4), (2, 2))),
        "in_c": scatter_about(key_of[3], (BATCH, DRAFT, GROUPS * STATE), 0.125, 0.75, ((0, 4), (1, 4), (2, 2))),
        "step_size": jnp.clip(jnp.exp(math.log(1.0) - 3.9171631 * jax.random.uniform(key_of[4], (BATCH, DRAFT, HEADS), jnp.float32) ** level_of(key_of[4], (BATCH, DRAFT, HEADS), ((0, 4), (1, 4), (2, 2)), -0.2, 0.2)), 0.019897461, 1.0).astype(jnp.bfloat16),
        "decay_rate": jnp.clip(jnp.exp(math.log(1.0) - 4.6051702 * jax.random.uniform(key_of[5], (HEADS,), jnp.float32) ** level_of(key_of[5], (HEADS,), ((0, 2),), -0.2, 0.2)), 0.01, 1.0),
        "skip_weight": jnp.clip(0.5 + 1.0 * jax.random.uniform(key_of[6], (HEADS,), jnp.float32) ** level_of(key_of[6], (HEADS,), ((0, 2),), -0.2, 0.2), 0.5, 1.5),
        "norm_gain": jnp.clip(1.0 + 0.18 * jax.random.normal(key_of[7], (HEADS * HEAD_DIM,), jnp.float32), 0.1, 1.9),
        "ssm_state": scatter_about(key_of[8], (BATCH, HEADS, HEAD_DIM, STATE), 1.0, 6.0, ((0, 4), (1, 2), (3, 4))),
        "out_weight": scatter_about(key_of[9], (HEADS * HEAD_DIM, D), (HEADS * HEAD_DIM) ** -0.5, 0.125, ((0, 8),)),
        "queries": draw_queries(jax.random.fold_in(key_of[17], 71), 0),
        "draft_token_keys": scatter_about(key_of[11], (BATCH, DRAFT, KVHEADS * ATT_DIM), 1.0, 6.0, ((0, 4), (1, 4), (2, 2))),
        "draft_values": scatter_about(key_of[12], (BATCH, DRAFT, KVHEADS * ATT_DIM), 1.0, 6.0, ((0, 4), (1, 4), (2, 2))),
        "cached_key_rows": draw_cached_key_rows(jax.random.fold_in(key_of[17], 71), 0),
        "cache_values": scatter_about(key_of[14], (BATCH, CACHE, KVHEADS * ATT_DIM), 1.0, 6.0, ((0, 4), (1, 4), (2, 2))),
        "cache_len": with_ends(jax.random.randint(key_of[15], (BATCH,), 2, CACHE + 1), jax.random.fold_in(key_of[15], 1), 2, CACHE).astype(jnp.int32),
        "accepted": with_ends(jax.random.randint(key_of[16], (BATCH,), 0, DRAFT + 1), jax.random.fold_in(key_of[16], 1), 0, DRAFT).astype(jnp.int32),
    }


PRECISE = lax.Precision.HIGHEST
EPSILON = 1e-05
MASKED = -1e+30

def attend_one(inputs):
    query_matrix, new_keys, new_values, old_keys, old_values, valid_length = inputs
    draft_len = query_matrix.shape[0]
    kv_heads = new_keys.shape[1] // ATT_DIM
    per_kv = query_matrix.shape[1] // ATT_DIM // kv_heads
    cache_size = old_keys.shape[0]
    queries_f = query_matrix.astype(jnp.float32).reshape(draft_len, kv_heads, per_kv, ATT_DIM)
    keys_f = jnp.concatenate([old_keys, new_keys], axis=0).astype(jnp.float32).reshape(cache_size + draft_len, kv_heads, ATT_DIM)
    values_f = jnp.concatenate([old_values, new_values], axis=0).astype(jnp.float32).reshape(cache_size + draft_len, kv_heads, ATT_DIM)
    scores = jnp.einsum('sgqd,kgd->gsqk', queries_f, keys_f, precision=PRECISE) * ATT_DIM ** (-0.5)
    key_pos = jnp.arange(cache_size + draft_len)
    query_pos = jnp.arange(draft_len)
    allowed = jnp.where(key_pos[None, :] < cache_size, key_pos[None, :] < valid_length, key_pos[None, :] - cache_size <= query_pos[:, None])
    allowed = allowed[None, :, None, :]
    scores = jnp.where(allowed, scores, MASKED)
    row_peak = lax.optimization_barrier(jnp.max(scores, axis=-1, keepdims=True))
    probs = jnp.where(allowed, jnp.exp(scores - row_peak), 0.0)
    totals = lax.optimization_barrier(jnp.sum(probs, axis=-1))
    rounded = lax.optimization_barrier(probs.astype(jnp.bfloat16)).astype(jnp.float32)
    numer = jnp.einsum('gsqk,kgd->gsqd', rounded, values_f, precision=PRECISE)
    context = numer / totals[..., None]
    return jnp.transpose(context, (1, 0, 2, 3)).reshape(draft_len, kv_heads * per_kv * ATT_DIM).astype(jnp.bfloat16)

def reference(mamba_input, gate_input, in_b, in_c, step_size, decay_rate, skip_weight, norm_gain, ssm_state, out_weight, queries, draft_token_keys, draft_values, cached_key_rows, cache_values, cache_len, accepted):
    batch, draft_len, feature_width = mamba_input.shape
    head_count = decay_rate.shape[0]
    group_count = in_b.shape[2] // STATE
    per_group = head_count // group_count
    feature_values = mamba_input.astype(jnp.float32).reshape(batch, draft_len, head_count, HEAD_DIM)
    step_sizes = step_size.astype(jnp.float32)
    inflow = jnp.repeat(in_b.astype(jnp.float32).reshape(batch, draft_len, group_count, STATE), per_group, axis=2)
    readout = jnp.repeat(in_c.astype(jnp.float32).reshape(batch, draft_len, group_count, STATE), per_group, axis=2)
    log_decay = -step_sizes * decay_rate[None, None, :]
    running = jnp.cumsum(log_decay, axis=1)
    position = jnp.arange(draft_len)
    causal = (position[:, None] >= position[None, :])[None, :, :, None]
    log_gaps = jnp.where(causal, running[:, :, None, :] - running[:, None, :, :], 0.0)
    decays = jnp.where(causal, jnp.exp(log_gaps), 0.0)
    affinity = jnp.einsum('bshn,brhn->bsrh', readout, inflow, precision=PRECISE)
    mixing = affinity * decays * step_sizes[:, None, :, :]
    within = jnp.einsum('bsrh,brhp->bshp', mixing, feature_values, precision=PRECISE)
    start_state = ssm_state.astype(jnp.float32)
    carried = jnp.einsum('bshn,bhpn->bshp', readout, start_state, precision=PRECISE) * jnp.exp(running)[..., None]
    mixed = within + carried + skip_weight[None, None, :, None] * feature_values
    gated = mixed.reshape(batch, draft_len, feature_width) * jax.nn.silu(gate_input.astype(jnp.float32))
    grouped = gated.reshape(batch, draft_len, group_count, feature_width // group_count)
    mean_sq = lax.optimization_barrier(jnp.mean(grouped * grouped, axis=-1, keepdims=True))
    normed = (grouped * lax.rsqrt(mean_sq + EPSILON)).reshape(batch, draft_len, feature_width) * norm_gain
    normed = normed.astype(jnp.bfloat16)
    blocks = N_HEAD * N_TOK
    block_rows = feature_width // blocks
    pieces = jnp.transpose(normed.reshape(batch * draft_len, blocks, block_rows), (1, 0, 2))
    weight_blocks = out_weight.reshape(blocks, block_rows, out_weight.shape[1])

    def add_block(accum, pair):
        piece, weight = pair
        part_sum = jnp.dot(piece, weight, preferred_element_type=jnp.float32)
        part_sum = lax.optimization_barrier(part_sum.astype(jnp.bfloat16)).astype(jnp.float32)
        return (accum + part_sum, None)
    summed_total, unused = lax.scan(add_block, jnp.zeros((batch * draft_len, out_weight.shape[1]), jnp.float32), (pieces, weight_blocks))
    mamba_out = jnp.transpose(summed_total.reshape(batch, draft_len, out_weight.shape[1]), (1, 0, 2)).astype(jnp.bfloat16)
    alive = (position[None, :] < accepted[:, None])[..., None]
    end_log = lax.optimization_barrier(jnp.sum(jnp.where(alive, log_decay, 0.0), axis=1))
    weights = jnp.where(alive, jnp.exp(jnp.where(alive, end_log[:, None, :] - running, 0.0)) * step_sizes, 0.0)
    committed = jnp.exp(end_log)[..., None, None] * start_state + jnp.einsum('bsh,bshp,bshn->bhpn', weights, feature_values, inflow, precision=PRECISE)
    committed_state = committed.astype(jnp.bfloat16)
    attn_context = lax.map(attend_one, (queries, draft_token_keys, draft_values, cached_key_rows, cache_values, cache_len))
    return (mamba_out, attn_context, committed_state)
```

```python
import functools
import jax
import jax.numpy as jnp
from jax import lax
from jax.experimental import pallas as pl
from jax.experimental.pallas import tpu as pltpu
from jax.sharding import PartitionSpec as P

EPSILON = 1e-05
MASKED = -1e30
FLOOR = -1e29
MESH = pl.DeviceIdType.MESH
F32 = jnp.float32
BF16 = jnp.bfloat16
NT = (((1,), (1,)), ((), ()))


def dot(a, b):
    return jnp.dot(a, b, preferred_element_type=F32)


def iota(shape, dim):
    return lax.broadcasted_iota(jnp.int32, shape, dim)


def kernel(
    dims,
    x_in, z_in, b_in, c_in, dt_in, st_in, q_in, k_in, v_in, w_in,
    dk_ref, dv_ref, gain_ref, rate_ref, skip_ref, len_ref, acc_ref,
    out_ref, ctx_ref, com_ref,
    x_l, z_l, b_l, c_l, dt_l, st_l, q_l, k_v, v_v, w_v,
    ss_l, cm_s, cm_l, n_s, n_l, stat_l, part, rs_l,
    send, recv, rs_send, rs_recv, local,
):
    n_head, n_tok, seqs, block, heads, chunks = dims
    group = n_head * n_tok
    tok = lax.axis_index("tok")
    head = lax.axis_index("head")
    me = head * n_tok + tok
    draft = block * n_tok
    width = x_l.shape[2]
    own = heads // n_tok
    size = width // own
    state = st_l.shape[1]
    cols = state // n_tok
    att = k_v.shape[2]
    per_kv = q_l.shape[2] // att
    cache = k_v.shape[1]
    rows = seqs * draft
    each = rows // group
    out_cols = w_v.shape[1]
    span = out_cols // chunks

    def place(index, unit):
        return pl.ds(pl.multiple_of(index * unit, unit), unit)

    barrier = pltpu.get_barrier_semaphore()
    for o in range(1, group):
        peer = lax.rem(me + o, group)
        pl.semaphore_signal(
            barrier, inc=1,
            device_id={"head": peer // n_tok, "tok": lax.rem(peer, n_tok)},
            device_id_type=MESH,
        )

    mine = place(tok, block)
    locals_ = [
        (x_in.at[:, :, place(tok, width)], x_l.at[:, mine, :]),
        (z_in.at[:, :, place(tok, width)], z_l.at[:, mine, :]),
        (b_in, b_l.at[:, mine, :]),
        (c_in, c_l.at[:, mine, :]),
        (dt_in, dt_l.at[:, mine, :]),
        (st_in.at[:, :, place(tok, width)], st_l.at[:, place(tok, cols), :]),
        (q_in, q_l.at[:, mine, :]),
        (w_in, w_v),
        (k_in, k_v),
        (v_in, v_v),
    ]
    held = [
        pltpu.make_async_copy(src, dst, local.at[i]) for i, (src, dst) in enumerate(locals_)
    ]
    for copy in held:
        copy.start()

    pl.semaphore_wait(barrier, group - 1)

    def remote(kind, o, src, dst):
        return pltpu.make_async_remote_copy(
            src_ref=src, dst_ref=dst,
            send_sem=send.at[kind, o], recv_sem=recv.at[kind, o],
            device_id={"tok": lax.rem(tok + o, n_tok)}, device_id_type=MESH,
        )

    started = []

    def ship(kind, o, src, dst):
        copy = remote(kind, o, src, dst)
        copy.start()
        started.append(copy)

    first = {}
    for o in range(1, n_tok):
        to = lax.rem(tok + o, n_tok)
        pairs = [
            (dt_in, dt_l.at[:, mine, :]),
            (b_in, b_l.at[:, mine, :]),
            (c_in, c_l.at[:, mine, :]),
            (x_in.at[:, :, place(to, width)], x_l.at[:, mine, :]),
            (st_in.at[:, :, place(to, width)], st_l.at[:, place(tok, cols), :]),
            (z_in.at[:, :, place(to, width)], z_l.at[:, mine, :]),
        ]
        for kind, (src, dst) in enumerate(pairs):
            ship(kind, o, src, dst)
            first[kind, o] = started[-1]
    for o in range(1, n_tok):
        ship(6, o, q_in, q_l.at[:, mine, :])
        first[6, o] = started[-1]

    for copy in held[:6]:
        copy.wait()
    for kind in range(6):
        for o in range(1, n_tok):
            first[kind, o].wait_recv()

    lane = iota((1, width), 1)
    rate_x = jnp.zeros((1, width), F32)
    skip_x = jnp.zeros((1, width), F32)
    for h in range(own):
        inside = (lane >= h * size) & (lane < (h + 1) * size)
        rate_x = jnp.where(inside, rate_ref[tok * own + h], rate_x)
        skip_x = jnp.where(inside, skip_ref[tok * own + h], skip_x)
    offset = iota((heads, width), 1) - (iota((heads, width), 0) - tok * own) * size
    pick = ((offset >= 0) & (offset < size)).astype(F32).astype(BF16)
    causal = iota((draft, draft), 0) >= iota((draft, draft), 1)
    lower = causal.astype(F32).astype(BF16)

    gated = []
    saved = []
    for s in range(seqs):
        x = x_l[s].astype(F32)
        z = z_l[s].astype(F32)
        b = b_l[s]
        c = c_l[s]
        st = st_l[s]
        dtx = dot(dt_l[s], pick)
        run = -rate_x * dot(lower, dtx.astype(BF16))
        scaled = (x * dtx * jnp.exp(-run)).astype(BF16)
        mix = lax.dot_general(c, b, NT, preferred_element_type=F32)
        mix = jnp.where(causal, mix, 0.0).astype(BF16)
        y = jnp.exp(run) * (dot(mix, scaled) + dot(c, st)) + skip_x * x
        gated.append(y * z / (1.0 + jnp.exp(-z)))
        saved.append((x, dtx, run))
    gated = jnp.concatenate(gated, axis=0)
    sums = jnp.sum(gated * gated, axis=1, keepdims=True)
    eye = iota((rows, rows), 0) == iota((rows, rows), 1)
    sum_row = jnp.sum(jnp.where(eye, sums, 0.0), axis=0, keepdims=True)
    ss_l[tok] = jnp.broadcast_to(sum_row, (8, rows))
    for o in range(1, n_tok):
        ship(7, o, ss_l.at[tok], ss_l.at[tok])
        first[7, o] = started[-1]

    for s in range(seqs):
        x, dtx, run = saved[s]
        alive = iota((draft, width), 0) < acc_ref[s]
        end = -rate_x * jnp.sum(jnp.where(alive, dtx, 0.0), axis=0, keepdims=True)
        weight = jnp.where(alive, jnp.exp(jnp.where(alive, end - run, 0.0)) * dtx, 0.0)
        flow = b_l[s].astype(F32).T.astype(BF16)
        new = jnp.exp(end) * st_l[s].astype(F32) + dot(flow, (x * weight).astype(BF16))
        cm_s[s] = new.astype(BF16)

    for o in range(1, n_tok):
        first[7, o].wait_recv()
    totals = jnp.zeros((1, rows), F32)
    for t in range(n_tok):
        totals = totals + ss_l[t][0:1, :]
    col = jnp.sum(jnp.where(eye, totals, 0.0), axis=1, keepdims=True)
    gain = gain_ref[:, place(tok, width)]
    normed = gated * lax.rsqrt(col / (width * n_tok) + EPSILON) * gain
    swap = None
    for s in range(seqs):
        k = iota((rows, rows), 1) - s * draft
        hit = (k >= 0) & (k < draft) & (k * seqs + s == iota((rows, rows), 0))
        swap = hit if swap is None else swap | hit
    normed = dot(swap.astype(F32).astype(BF16), normed.astype(BF16)).astype(BF16)

    held[7].wait()
    tile = min(512, span)
    rs = {}
    for ch in range(chunks):
        for start in range(ch * span, (ch + 1) * span, tile):
            val = dot(normed, w_v[:, start : start + tile]).astype(BF16)
            for g in range(group):
                part[g, :, start : start + tile] = val[g * each : (g + 1) * each]
        for o in range(1, group):
            peer = lax.rem(me + o, group)
            piece = pl.ds(ch * span, span)
            copy = pltpu.make_async_remote_copy(
                src_ref=part.at[peer, :, piece], dst_ref=rs_l.at[o, :, piece],
                send_sem=rs_send.at[ch, o], recv_sem=rs_recv.at[ch, o],
                device_id={"head": peer // n_tok, "tok": lax.rem(peer, n_tok)},
                device_id_type=MESH,
            )
            copy.start()
            rs[ch, o] = copy

    for o in range(1, n_tok):
        first[6, o].wait_recv()
    held[6].wait()
    held[8].wait()
    held[9].wait()
    scale = att ** (-0.5)
    m_rows = per_kv * draft
    big = iota((m_rows, m_rows), 0) == iota((m_rows, m_rows), 1)
    position = tok * cache + iota((1, cache), 1)
    draft_at = tok * block + iota((draft, block), 1)
    seen = draft_at <= iota((draft, block), 0)
    seen = jnp.concatenate([seen.astype(F32)] * per_kv, axis=0) > 0.5
    for s in range(seqs):
        q = jnp.concatenate([q_l[s, :, h * att : (h + 1) * att] for h in range(per_kv)], axis=0)
        old = lax.dot_general(q, k_v[s], NT, preferred_element_type=F32)
        old = jnp.where(position < len_ref[s], old, MASKED)
        new = lax.dot_general(q, dk_ref[s], NT, preferred_element_type=F32)
        new = jnp.where(seen, new, MASKED)
        peak = jnp.maximum(
            jnp.max(old, axis=1, keepdims=True), jnp.max(new, axis=1, keepdims=True)
        )
        peak = jnp.maximum(peak, FLOOR)
        old = jnp.exp((old - peak) * scale)
        new = jnp.exp((new - peak) * scale)
        total = jnp.sum(old, axis=1, keepdims=True) + jnp.sum(new, axis=1, keepdims=True)
        numer = dot(old.astype(BF16), v_v[s]) + dot(new.astype(BF16), dv_ref[s])
        safe = jnp.maximum(total, 1e-30)
        ctx = (numer / safe).astype(BF16)
        level = jnp.where(total > 0.0, peak * scale + jnp.log(safe), MASKED)
        for h in range(per_kv):
            n_s[s, h] = ctx[h * draft : (h + 1) * draft]
        stat_l[tok, s : s + 1, :] = jnp.sum(jnp.where(big, level, 0.0), axis=0, keepdims=True)
    for o in range(1, n_tok):
        to = lax.rem(tok + o, n_tok)
        ship(8, o, stat_l.at[tok], stat_l.at[tok])
        first[8, o] = started[-1]
        ship(9, o, n_s.at[:, :, place(to, block), :], n_l.at[tok])
        first[9, o] = started[-1]
    for o in range(1, n_tok):
        to = lax.rem(tok + o, n_tok)
        ship(10, o, cm_s.at[:, place(to, cols), :], cm_l.at[:, :, place(tok, width)])
        first[10, o] = started[-1]
    n_l[tok] = n_s[:, :, mine, :]
    cm_l[:, :, place(tok, width)] = cm_s[:, place(tok, cols), :]

    for ch in range(chunks):
        for o in range(1, group):
            rs[ch, o].wait_recv()
        for start in range(ch * span, (ch + 1) * span, tile):
            acc = part[me, :, start : start + tile].astype(F32)
            for o in range(1, group):
                acc = acc + rs_l[o, :, start : start + tile].astype(F32)
            out_ref[:, start : start + tile] = acc.astype(BF16)

    for o in range(1, n_tok):
        first[8, o].wait_recv()
        first[9, o].wait_recv()
    m_own = per_kv * block
    lanes = iota((m_own, m_rows), 1)
    r = iota((m_own, m_rows), 0)
    want = None
    for h in range(per_kv):
        t = r - h * block
        hit = (t >= 0) & (t < block) & (lanes == h * draft + tok * block + t)
        want = hit if want is None else want | hit
    for s in range(seqs):
        levels = [
            jnp.sum(jnp.where(want, stat_l[t][s : s + 1, :], 0.0), axis=1, keepdims=True)
            for t in range(n_tok)
        ]
        top = functools.reduce(jnp.maximum, levels)
        weights = [jnp.exp(level - top) for level in levels]
        den = functools.reduce(jnp.add, weights)
        acc = jnp.zeros((m_own, att), F32)
        for t in range(n_tok):
            got = jnp.concatenate([n_l[t, s, h].astype(F32) for h in range(per_kv)], axis=0)
            acc = acc + weights[t] * got
        acc = (acc / den).astype(BF16)
        for h in range(per_kv):
            ctx_ref[s, :, h * att : (h + 1) * att] = acc[h * block : (h + 1) * block]

    for o in range(1, n_tok):
        first[10, o].wait_recv()
    com_ref[...] = cm_l[...]
    for copy in started:
        copy.wait_send()
    for copy in rs.values():
        copy.wait_send()


def body(
    mamba_input, gate_input, in_b, in_c, step_size, decay_rate, skip_weight, norm_gain,
    ssm_state, out_weight, queries, draft_token_keys, draft_values, cached_key_rows,
    cache_values, cache_len, accepted,
):
    n_tok = lax.axis_size("tok")
    n_head = lax.axis_size("head")
    group = n_head * n_tok
    seqs, block, features = mamba_input.shape
    heads = decay_rate.shape[0]
    size = features // heads
    cols = ssm_state.shape[3]
    state = cols * n_tok
    draft = block * n_tok
    width = features // n_tok
    att = draft_token_keys.shape[2]
    per_kv = queries.shape[2] // att
    cache = cached_key_rows.shape[1]
    out_cols = out_weight.shape[1]
    rows = seqs * draft
    each = rows // group
    chunks = 2
    turned = jnp.transpose(ssm_state, (0, 3, 1, 2)).reshape(seqs, cols, features)
    anys = [pl.BlockSpec(memory_space=pl.ANY)] * 10
    vmems = [pl.BlockSpec(memory_space=pltpu.VMEM)] * 3
    smems = [pl.BlockSpec(memory_space=pltpu.SMEM)] * 4
    out, ctx, com = pl.pallas_call(
        functools.partial(kernel, (n_head, n_tok, seqs, block, heads, chunks)),
        out_shape=(
            jax.ShapeDtypeStruct((each, out_cols), BF16),
            jax.ShapeDtypeStruct((seqs, block, per_kv * att), BF16),
            jax.ShapeDtypeStruct((seqs, cols, features), BF16),
        ),
        in_specs=anys + vmems + smems,
        out_specs=[pl.BlockSpec(memory_space=pltpu.VMEM)] * 3,
        scratch_shapes=[
            pltpu.VMEM((seqs, draft, width), BF16),
            pltpu.VMEM((seqs, draft, width), BF16),
            pltpu.VMEM((seqs, draft, state), BF16),
            pltpu.VMEM((seqs, draft, state), BF16),
            pltpu.VMEM((seqs, draft, heads), BF16),
            pltpu.VMEM((seqs, state, width), BF16),
            pltpu.VMEM((seqs, draft, per_kv * att), BF16),
            pltpu.VMEM((seqs, cache, att), BF16),
            pltpu.VMEM((seqs, cache, att), BF16),
            pltpu.VMEM(out_weight.shape, BF16),
            pltpu.VMEM((n_tok, 8, rows), F32),
            pltpu.VMEM((seqs, state, width), BF16),
            pltpu.VMEM((seqs, cols, features), BF16),
            pltpu.VMEM((seqs, per_kv, draft, att), BF16),
            pltpu.VMEM((n_tok, seqs, per_kv, block, att), BF16),
            pltpu.VMEM((n_tok, seqs, per_kv * draft), F32),
            pltpu.VMEM((group, each, out_cols), BF16),
            pltpu.VMEM((group, each, out_cols), BF16),
            pltpu.SemaphoreType.DMA((11, n_tok)),
            pltpu.SemaphoreType.DMA((11, n_tok)),
            pltpu.SemaphoreType.DMA((chunks, group)),
            pltpu.SemaphoreType.DMA((chunks, group)),
            pltpu.SemaphoreType.DMA((10,)),
        ],
        compiler_params=pltpu.CompilerParams(
            collective_id=0, has_side_effects=True, vmem_limit_bytes=48 * 1024 * 1024
        ),
        name="hybrid",
    )(
        mamba_input, gate_input, in_b, in_c, step_size, turned, queries, cached_key_rows,
        cache_values, out_weight, draft_token_keys, draft_values,
        norm_gain.reshape(1, features), decay_rate, skip_weight, cache_len, accepted,
    )
    mamba_out = out.reshape(draft // group, seqs, out_cols)
    committed = jnp.transpose(com.reshape(seqs, cols, heads, size), (0, 2, 3, 1))
    return (mamba_out, ctx, committed)


def solution(mesh):
    in_specs = (
        P("dp", "tok", "head"),
        P("dp", "tok", "head"),
        P("dp", "tok", "head"),
        P("dp", "tok", "head"),
        P("dp", "tok", "head"),
        P("head"),
        P("head"),
        P("head"),
        P("dp", "head", None, "tok"),
        P(("head", "tok"), None),
        P("dp", "tok", "head"),
        P("dp", "tok", "head"),
        P("dp", "tok", "head"),
        P("dp", "tok", "head"),
        P("dp", "tok", "head"),
        P("dp"),
        P("dp"),
    )
    out_specs = (
        P(("head", "tok"), "dp", None),
        P("dp", "tok", "head"),
        P("dp", "head", None, "tok"),
    )
    return jax.shard_map(body, mesh=mesh, in_specs=in_specs, out_specs=out_specs, check_vma=False)
```

```python
import functools
import jax
import jax.numpy as jnp
from jax import lax
from jax.experimental import pallas as pl
from jax.experimental.pallas import tpu as pltpu
from jax.sharding import PartitionSpec as P

EPSILON = 1e-05
MASKED = -1e30
FLOOR = -1e29
MESH = pl.DeviceIdType.MESH
F32 = jnp.float32
BF16 = jnp.bfloat16
NT = (((1,), (1,)), ((), ()))


def dot(a, b):
    return jnp.dot(a, b, preferred_element_type=F32)


def iota(shape, dim):
    return lax.broadcasted_iota(jnp.int32, shape, dim)


def kernel(
    dims,
    x_in, z_in, b_in, c_in, dt_in, st_in, q_in, k_in, v_in, w_in,
    dk_in, dv_in, gain_in, rate_ref, skip_ref, len_ref, acc_ref,
    out_ref, ctx_ref, com_ref,
    x_l, z_l, b_l, c_l, dt_l, st_l, q_l, k_v, v_v, w_v,
    ss_l, cm_s, cm_l, n_s, n_l, stat_l, part, rs_l,
    dk_ref, dv_ref, gain_ref, raw_v, turn_v, pair_l, red,
    send, recv, rs_send, rs_recv, pair_send, pair_recv, local,
):
    n_head, n_tok, seqs, block, heads, chunks = dims
    group = n_head * n_tok
    tok = lax.axis_index("tok")
    head = lax.axis_index("head")
    me = head * n_tok + tok
    draft = block * n_tok
    width = x_l.shape[2]
    own = heads // n_tok
    size = width // own
    state = st_l.shape[1]
    cols = state // n_tok
    att = k_v.shape[2]
    per_kv = q_l.shape[2] // att
    cache = k_v.shape[1]
    rows = seqs * draft
    each = rows // group
    out_cols = w_v.shape[1]
    span = out_cols // chunks

    def place(index, unit):
        return pl.ds(pl.multiple_of(index * unit, unit), unit)

    barrier = pltpu.get_barrier_semaphore()
    for o in range(1, group):
        peer = lax.rem(me + o, group)
        pl.semaphore_signal(
            barrier, inc=1,
            device_id={"head": peer // n_tok, "tok": lax.rem(peer, n_tok)},
            device_id_type=MESH,
        )

    mine = place(tok, block)
    locals_ = [
        (x_in.at[:, :, place(tok, width)], x_l.at[:, mine, :]),
        (z_in.at[:, :, place(tok, width)], z_l.at[:, mine, :]),
        (b_in, b_l.at[:, mine, :]),
        (c_in, c_l.at[:, mine, :]),
        (dt_in, dt_l.at[:, mine, :]),
        (st_in, raw_v),
        (q_in, q_l.at[:, mine, :]),
        (w_in, w_v),
        (k_in, k_v),
        (v_in, v_v),
        (dk_in, dk_ref),
        (dv_in, dv_ref),
        (gain_in, gain_ref),
    ]
    held = [
        pltpu.make_async_copy(src, dst, local.at[i]) for i, (src, dst) in enumerate(locals_)
    ]
    for copy in held:
        copy.start()

    held[5].wait()
    for s in range(seqs):
        turn_v[s] = jnp.concatenate(
            [raw_v[s, h].astype(F32) for h in range(heads)], axis=1
        ).astype(BF16)
    st_l[:, place(tok, cols), :] = turn_v[:, :, place(tok, width)]

    pl.semaphore_wait(barrier, group - 1)

    def remote(kind, o, src, dst):
        return pltpu.make_async_remote_copy(
            src_ref=src, dst_ref=dst,
            send_sem=send.at[kind, o], recv_sem=recv.at[kind, o],
            device_id={"tok": lax.rem(tok + o, n_tok)}, device_id_type=MESH,
        )

    started = []

    def ship(kind, o, src, dst):
        copy = remote(kind, o, src, dst)
        copy.start()
        started.append(copy)

    first = {}
    for o in range(1, n_tok):
        to = lax.rem(tok + o, n_tok)
        pairs = [
            (dt_in, dt_l.at[:, mine, :]),
            (b_in, b_l.at[:, mine, :]),
            (c_in, c_l.at[:, mine, :]),
            (x_in.at[:, :, place(to, width)], x_l.at[:, mine, :]),
            (turn_v.at[:, :, place(to, width)], st_l.at[:, place(tok, cols), :]),
            (z_in.at[:, :, place(to, width)], z_l.at[:, mine, :]),
        ]
        for kind, (src, dst) in enumerate(pairs):
            ship(kind, o, src, dst)
            first[kind, o] = started[-1]
    for o in range(1, n_tok):
        ship(6, o, q_in, q_l.at[:, mine, :])
        first[6, o] = started[-1]

    lane = iota((1, width), 1)
    rate_x = jnp.zeros((1, width), F32)
    skip_x = jnp.zeros((1, width), F32)
    for h in range(own):
        inside = (lane >= h * size) & (lane < (h + 1) * size)
        rate_x = jnp.where(inside, rate_ref[tok * own + h], rate_x)
        skip_x = jnp.where(inside, skip_ref[tok * own + h], skip_x)
    offset = iota((heads, width), 1) - (iota((heads, width), 0) - tok * own) * size
    pick = ((offset >= 0) & (offset < size)).astype(F32).astype(BF16)
    causal = iota((draft, draft), 0) >= iota((draft, draft), 1)
    lower = causal.astype(F32).astype(BF16)

    eye = iota((rows, rows), 0) == iota((rows, rows), 1)
    source = iota((1, rows), 1)
    target = jnp.zeros((1, rows), jnp.int32)
    per = draft // group
    for s in range(seqs):
        for g in range(group):
            start = s * draft + g * per
            base = (g % 2) * (rows // 2) + (g // 2) * each + s
            inside = (source >= start) & (source < start + per)
            target = jnp.where(inside, (source - start) * seqs + base, target)
    swap = (iota((rows, rows), 0) == target).astype(F32).astype(BF16)

    for copy in held[:5]:
        copy.wait()
    for kind in range(6):
        for o in range(1, n_tok):
            first[kind, o].wait_recv()

    gated = []
    saved = []
    for s in range(seqs):
        x = x_l[s].astype(F32)
        z = z_l[s].astype(F32)
        b = b_l[s]
        c = c_l[s]
        st = st_l[s]
        dtx = dot(dt_l[s], pick)
        run = -rate_x * dot(lower, dtx.astype(BF16))
        scaled = (x * dtx * jnp.exp(-run)).astype(BF16)
        mix = lax.dot_general(c, b, NT, preferred_element_type=F32)
        mix = jnp.where(causal, mix, 0.0).astype(BF16)
        y = jnp.exp(run) * (dot(mix, scaled) + dot(c, st)) + skip_x * x
        gated.append(y * z / (1.0 + jnp.exp(-z)))
        saved.append((x, dtx, run))
    gated = jnp.concatenate(gated, axis=0)
    sums = jnp.sum(gated * gated, axis=1, keepdims=True)
    sum_row = jnp.sum(jnp.where(eye, sums, 0.0), axis=0, keepdims=True)
    ss_l[tok] = jnp.broadcast_to(sum_row, (8, rows))
    for o in range(1, n_tok):
        ship(7, o, ss_l.at[tok], ss_l.at[tok])
        first[7, o] = started[-1]

    for s in range(seqs):
        x, dtx, run = saved[s]
        alive = iota((draft, width), 0) < acc_ref[s]
        end = -rate_x * jnp.sum(jnp.where(alive, dtx, 0.0), axis=0, keepdims=True)
        weight = jnp.where(alive, jnp.exp(jnp.where(alive, end - run, 0.0)) * dtx, 0.0)
        flow = b_l[s].astype(F32).T.astype(BF16)
        new = jnp.exp(end) * st_l[s].astype(F32) + dot(flow, (x * weight).astype(BF16))
        cm_s[s] = new.astype(BF16)

    for o in range(1, n_tok):
        first[7, o].wait_recv()
    totals = jnp.zeros((1, rows), F32)
    for t in range(n_tok):
        totals = totals + ss_l[t][0:1, :]
    col = jnp.sum(jnp.where(eye, totals, 0.0), axis=1, keepdims=True)
    held[12].wait()
    gain = gain_ref[:, place(tok, width)]
    normed = gated * lax.rsqrt(col / (width * n_tok) + EPSILON) * gain
    normed = dot(swap, normed.astype(BF16)).astype(BF16)

    held[7].wait()
    tile = min(512, span)
    rs = {}
    pairs = []
    half = group // 2
    side = lax.rem(tok, 2)
    lines = n_tok // 2
    slot = head * lines + tok // 2

    def forward(ch):
        pairs[ch].wait_recv()
        piece = pl.ds(ch * span, span)
        red[:, :, piece] = (
            part[side, :, :, piece].astype(F32) + pair_l[:, :, piece].astype(F32)
        ).astype(BF16)
        for o in range(1, half):
            peer = lax.rem(slot + o, half)
            copy = pltpu.make_async_remote_copy(
                src_ref=red.at[peer, :, piece], dst_ref=rs_l.at[o, :, piece],
                send_sem=rs_send.at[ch, o], recv_sem=rs_recv.at[ch, o],
                device_id={"head": peer // lines, "tok": lax.rem(peer, lines) * 2 + side},
                device_id_type=MESH,
            )
            copy.start()
            rs[ch, o] = copy

    for ch in range(chunks):
        for start in range(ch * span, (ch + 1) * span, tile):
            val = dot(normed, w_v[:, start : start + tile]).astype(BF16)
            for p in range(2):
                for g in range(half):
                    at = (p * half + g) * each
                    part[p, g, :, start : start + tile] = val[at : at + each]
        piece = pl.ds(ch * span, span)
        copy = pltpu.make_async_remote_copy(
            src_ref=part.at[1 - side, :, :, piece], dst_ref=pair_l.at[:, :, piece],
            send_sem=pair_send.at[ch], recv_sem=pair_recv.at[ch],
            device_id={"tok": tok + 1 - 2 * side}, device_id_type=MESH,
        )
        copy.start()
        pairs.append(copy)
        if ch > 0:
            forward(ch - 1)
    forward(chunks - 1)

    for o in range(1, n_tok):
        first[6, o].wait_recv()
    held[6].wait()
    held[8].wait()
    for copy in held[9:12]:
        copy.wait()
    scale = att ** (-0.5)
    m_rows = per_kv * draft
    big = iota((m_rows, m_rows), 0) == iota((m_rows, m_rows), 1)
    position = tok * cache + iota((1, cache), 1)
    draft_at = tok * block + iota((draft, block), 1)
    seen = draft_at <= iota((draft, block), 0)
    seen = jnp.concatenate([seen.astype(F32)] * per_kv, axis=0) > 0.5
    for s in range(seqs):
        q = jnp.concatenate([q_l[s, :, h * att : (h + 1) * att] for h in range(per_kv)], axis=0)
        old = lax.dot_general(q, k_v[s], NT, preferred_element_type=F32)
        old = jnp.where(position < len_ref[s], old, MASKED)
        new = lax.dot_general(q, dk_ref[s], NT, preferred_element_type=F32)
        new = jnp.where(seen, new, MASKED)
        peak = jnp.maximum(
            jnp.max(old, axis=1, keepdims=True), jnp.max(new, axis=1, keepdims=True)
        )
        peak = jnp.maximum(peak, FLOOR)
        old = jnp.exp((old - peak) * scale)
        new = jnp.exp((new - peak) * scale)
        total = jnp.sum(old, axis=1, keepdims=True) + jnp.sum(new, axis=1, keepdims=True)
        numer = dot(old.astype(BF16), v_v[s]) + dot(new.astype(BF16), dv_ref[s])
        safe = jnp.maximum(total, 1e-30)
        ctx = (numer / safe).astype(BF16)
        level = jnp.where(total > 0.0, peak * scale + jnp.log(safe), MASKED)
        for h in range(per_kv):
            n_s[s, h] = ctx[h * draft : (h + 1) * draft]
        stat_l[tok, s : s + 1, :] = jnp.sum(jnp.where(big, level, 0.0), axis=0, keepdims=True)
    for o in range(1, n_tok):
        to = lax.rem(tok + o, n_tok)
        ship(8, o, stat_l.at[tok], stat_l.at[tok])
        first[8, o] = started[-1]
        ship(9, o, n_s.at[:, :, place(to, block), :], n_l.at[tok])
        first[9, o] = started[-1]
    for o in range(1, n_tok):
        to = lax.rem(tok + o, n_tok)
        ship(10, o, cm_s.at[:, place(to, cols), :], cm_l.at[:, :, place(tok, width)])
        first[10, o] = started[-1]
    n_l[tok] = n_s[:, :, mine, :]
    cm_l[:, :, place(tok, width)] = cm_s[:, place(tok, cols), :]

    for ch in range(chunks):
        for o in range(1, half):
            rs[ch, o].wait_recv()
        for start in range(ch * span, (ch + 1) * span, tile):
            acc = red[slot, :, start : start + tile].astype(F32)
            for o in range(1, half):
                acc = acc + rs_l[o, :, start : start + tile].astype(F32)
            out_ref[:, start : start + tile] = acc.astype(BF16)

    for o in range(1, n_tok):
        first[8, o].wait_recv()
        first[9, o].wait_recv()
    m_own = per_kv * block
    lanes = iota((m_own, m_rows), 1)
    r = iota((m_own, m_rows), 0)
    want = None
    for h in range(per_kv):
        t = r - h * block
        hit = (t >= 0) & (t < block) & (lanes == h * draft + tok * block + t)
        want = hit if want is None else want | hit
    for s in range(seqs):
        levels = [
            jnp.sum(jnp.where(want, stat_l[t][s : s + 1, :], 0.0), axis=1, keepdims=True)
            for t in range(n_tok)
        ]
        top = functools.reduce(jnp.maximum, levels)
        weights = [jnp.exp(level - top) for level in levels]
        den = functools.reduce(jnp.add, weights)
        acc = jnp.zeros((m_own, att), F32)
        for t in range(n_tok):
            got = jnp.concatenate([n_l[t, s, h].astype(F32) for h in range(per_kv)], axis=0)
            acc = acc + weights[t] * got
        acc = (acc / den).astype(BF16)
        for h in range(per_kv):
            ctx_ref[s, :, h * att : (h + 1) * att] = acc[h * block : (h + 1) * block]

    for o in range(1, n_tok):
        first[10, o].wait_recv()
    for s in range(seqs):
        for h in range(heads):
            com_ref[s, h] = cm_l[s, :, h * size : (h + 1) * size]
    for copy in started:
        copy.wait_send()
    for copy in pairs + list(rs.values()):
        copy.wait_send()


def body(
    mamba_input, gate_input, in_b, in_c, step_size, decay_rate, skip_weight, norm_gain,
    ssm_state, out_weight, queries, draft_token_keys, draft_values, cached_key_rows,
    cache_values, cache_len, accepted,
):
    n_tok = lax.axis_size("tok")
    n_head = lax.axis_size("head")
    group = n_head * n_tok
    seqs, block, features = mamba_input.shape
    heads = decay_rate.shape[0]
    size = features // heads
    cols = ssm_state.shape[3]
    state = cols * n_tok
    draft = block * n_tok
    width = features // n_tok
    att = draft_token_keys.shape[2]
    per_kv = queries.shape[2] // att
    cache = cached_key_rows.shape[1]
    out_cols = out_weight.shape[1]
    rows = seqs * draft
    each = rows // group
    chunks = 4
    half = group // 2
    turned = jnp.transpose(ssm_state, (0, 1, 3, 2))
    anys = [pl.BlockSpec(memory_space=pl.ANY)] * 13
    smems = [pl.BlockSpec(memory_space=pltpu.SMEM)] * 4
    out, ctx, com = pl.pallas_call(
        functools.partial(kernel, (n_head, n_tok, seqs, block, heads, chunks)),
        out_shape=(
            jax.ShapeDtypeStruct((each, out_cols), BF16),
            jax.ShapeDtypeStruct((seqs, block, per_kv * att), BF16),
            jax.ShapeDtypeStruct((seqs, heads, cols, size), BF16),
        ),
        in_specs=anys + smems,
        out_specs=[pl.BlockSpec(memory_space=pltpu.VMEM)] * 3,
        scratch_shapes=[
            pltpu.VMEM((seqs, draft, width), BF16),
            pltpu.VMEM((seqs, draft, width), BF16),
            pltpu.VMEM((seqs, draft, state), BF16),
            pltpu.VMEM((seqs, draft, state), BF16),
            pltpu.VMEM((seqs, draft, heads), BF16),
            pltpu.VMEM((seqs, state, width), BF16),
            pltpu.VMEM((seqs, draft, per_kv * att), BF16),
            pltpu.VMEM((seqs, cache, att), BF16),
            pltpu.VMEM((seqs, cache, att), BF16),
            pltpu.VMEM(out_weight.shape, BF16),
            pltpu.VMEM((n_tok, 8, rows), F32),
            pltpu.VMEM((seqs, state, width), BF16),
            pltpu.VMEM((seqs, cols, features), BF16),
            pltpu.VMEM((seqs, per_kv, draft, att), BF16),
            pltpu.VMEM((n_tok, seqs, per_kv, block, att), BF16),
            pltpu.VMEM((n_tok, seqs, per_kv * draft), F32),
            pltpu.VMEM((2, half, each, out_cols), BF16),
            pltpu.VMEM((half, each, out_cols), BF16),
            pltpu.VMEM((seqs, block, att), BF16),
            pltpu.VMEM((seqs, block, att), BF16),
            pltpu.VMEM((1, features), F32),
            pltpu.VMEM((seqs, heads, cols, size), BF16),
            pltpu.VMEM((seqs, cols, features), BF16),
            pltpu.VMEM((half, each, out_cols), BF16),
            pltpu.VMEM((half, each, out_cols), BF16),
            pltpu.SemaphoreType.DMA((11, n_tok)),
            pltpu.SemaphoreType.DMA((11, n_tok)),
            pltpu.SemaphoreType.DMA((chunks, half)),
            pltpu.SemaphoreType.DMA((chunks, half)),
            pltpu.SemaphoreType.DMA((chunks,)),
            pltpu.SemaphoreType.DMA((chunks,)),
            pltpu.SemaphoreType.DMA((13,)),
        ],
        compiler_params=pltpu.CompilerParams(
            collective_id=0, has_side_effects=True, vmem_limit_bytes=67043328
        ),
        name="hybrid",
    )(
        mamba_input, gate_input, in_b, in_c, step_size, turned, queries, cached_key_rows,
        cache_values, out_weight, draft_token_keys, draft_values,
        norm_gain.reshape(1, features), decay_rate, skip_weight, cache_len, accepted,
    )
    mamba_out = out.reshape(draft // group, seqs, out_cols)
    committed = jnp.transpose(com, (0, 1, 3, 2))
    return (mamba_out, ctx, committed)


def solution(mesh):
    in_specs = (
        P("dp", "tok", "head"),
        P("dp", "tok", "head"),
        P("dp", "tok", "head"),
        P("dp", "tok", "head"),
        P("dp", "tok", "head"),
        P("head"),
        P("head"),
        P("head"),
        P("dp", "head", None, "tok"),
        P(("head", "tok"), None),
        P("dp", "tok", "head"),
        P("dp", "tok", "head"),
        P("dp", "tok", "head"),
        P("dp", "tok", "head"),
        P("dp", "tok", "head"),
        P("dp"),
        P("dp"),
    )
    out_specs = (
        P(("head", "tok"), "dp", None),
        P("dp", "tok", "head"),
        P("dp", "head", None, "tok"),
    )
    return jax.shard_map(body, mesh=mesh, in_specs=in_specs, out_specs=out_specs, check_vma=False)
```
